32 devices in a mesh: ens: 4 (over x, core), dp: 8 (over z, y).
Axes of the slice: x: 2, y: 2, z: 4, core: 2. Of those that a mesh axis runs over, the one named last changes fastest.
Arguments:
- features: bfloat16 [3072, 256], P('dp'), may hold values from -4 to 4
- reward: float32 [3072], P('dp'), may hold values from -16 to 16
- done: int32 [3072], P('dp'), may hold values 0 or 1
- value_next: float32 [3072], P('dp'), may hold values from -16 to 16
- value_now: float32 [3072], P('dp'), may hold values from -4 to 4
- w_in: bfloat16 [8, 256, 2048], P('ens'), may hold values from -0.375 to 0.375
- w_mid: bfloat16 [8, 2048, 2048], P('ens'), may hold values from -0.099121094 to 0.099121094
- biases: float32 [2, 8, 2048], P(None, 'ens'), may hold values from -3 to 3
- w_out: bfloat16 [8, 2048], P('ens'), may hold values from -0.011048543 to 0.011048543
Outputs:
- value_grad: float32 [3072], P('dp')
- d_in: float32 [256, 8, 2048], P('dp', 'ens')
- d_mid: float32 [2048, 8, 2048], P('dp', 'ens')
- d_bias: float32 [2, 8, 2048], P(None, 'ens', 'dp')
- d_out: float32 [8, 2048], P('ens', 'dp')
The draws below stay inside these ranges and needn't reach their ends.
All inputs are finite; a program needn't handle non-finite values. No bound on the sum of `done` on one device may be relied on, other than what follows from the above.
Results may differ from the reference program's by a relative error of at most 0.013.
Values may be sent and summed in bfloat16 or wider, within the bound.
A program may use at most 128 MiB of HBM per device.

```python
import jax
import jax.numpy as jnp
from jax import lax

IN = 256
H = 2048
ROWS_DEV = 384
HEADS = 8
TOTAL = 3072


def draw_w_out(key, part):
    sign_key = jax.random.fold_in(key, 11)
    scale_key = jax.random.fold_in(key, 12)
    sign_values = (2 * jax.random.randint(sign_key, (HEADS, H), 0, 2) - 1).astype(jnp.float32)
    lowest = 0.5
    magnitude = jax.random.uniform(scale_key, (HEADS, H), jnp.float32, lowest, 1.0)
    return (sign_values * magnitude * (0.5 * H ** (-0.5))).astype(jnp.bfloat16)


def plant(entries, own_key, least, top_value):
    longest = entries.shape.index(max(entries.shape))
    spots = []
    for shift in (0, 1):
        where = [jax.random.randint(jax.random.fold_in(own_key, axis), (), 0, length) for axis, length in enumerate(entries.shape)]
        where[longest] = (where[longest] + shift) % entries.shape[longest]
        spots.append(tuple(where))
    return entries.at[spots[0]].set(least).at[spots[1]].set(top_value)


def steps_of(rng, extent, cuts, low, top_value):
    loudness = 1.0
    for dim, shards_of in cuts:
        heights = jax.random.uniform(jax.random.fold_in(jax.random.fold_in(rng, 6), dim), (shards_of,), jnp.float32, low / len(cuts), top_value / len(cuts))
        loudness = loudness * jnp.repeat(jnp.exp(heights), extent[dim] // shards_of).reshape((-1,) + (1,) * (len(extent) - 1 - dim))
    return loudness


def gaussian(stream_key, extent, scale, limit, shards=(), dtype=jnp.bfloat16):
    result = scale * jax.random.normal(stream_key, extent, jnp.float32)
    if shards:
        result = result * steps_of(stream_key, extent, shards, -0.22, 0.18)
    return jnp.clip(result, -limit, limit).astype(dtype)


def setup_inputs(seed: int = 0) -> dict:
    arg_keys = jax.random.split(jax.random.key(seed), 10)
    return {
        "features": jnp.clip(jax.random.uniform(arg_keys[0], (TOTAL, IN), jnp.float32, -4.0, 4.0) * steps_of(arg_keys[0], (TOTAL, IN), ((0, 8),), -0.4, 0.0), -4.0, 4.0).astype(jnp.bfloat16),
        "reward": gaussian(arg_keys[1], (TOTAL,), 4.0, 16.0, ((0, 8),), jnp.float32),
        "done": plant((jax.random.randint(arg_keys[2], (TOTAL,), 0, 10) < 1).astype(jnp.int32), jax.random.fold_in(arg_keys[2], 1), 0, 1),
        "value_next": gaussian(arg_keys[3], (TOTAL,), 4.0, 16.0, ((0, 8),), jnp.float32),
        "value_now": gaussian(arg_keys[4], (TOTAL,), 0.5, 4.0, ((0, 8),), jnp.float32),
        "w_in": gaussian(arg_keys[5], (HEADS, IN, H), IN ** -0.5, 0.375, ((0, 4),)),
        "w_mid": jnp.clip(jax.random.uniform(arg_keys[6], (HEADS, H, H), jnp.float32, -0.099121094, 0.099121094) * steps_of(arg_keys[6], (HEADS, H, H), ((0, 4),), -0.4, 0.0), -0.099121094, 0.099121094).astype(jnp.bfloat16),
        "biases": gaussian(arg_keys[7], (2, HEADS, H), 0.5, 3.0, ((1, 4),), jnp.float32),
        "w_out": draw_w_out(jax.random.fold_in(arg_keys[9], 71), 0),
    }


def silu_slope(value):
    sig = jax.nn.sigmoid(value)
    return sig * (1.0 + value * (1.0 - sig))


def rounded(value):
    return lax.optimization_barrier(value.astype(jnp.bfloat16)).astype(jnp.float32)


def reference(features, reward, done, value_next, value_now, w_in, w_mid, biases, w_out):
    total = features.shape[0]
    blocks = total // ROWS_DEV
    width_in = features.shape[1]
    hidden = w_mid.shape[1]
    feat_blocks = features.reshape(blocks, ROWS_DEV, width_in)
    target = reward + 0.99 * (1.0 - done.astype(jnp.float32)) * value_next
    target_blocks = target.reshape(blocks, ROWS_DEV)
    high = lax.Precision.HIGHEST

    def head_pass(params):
        w_first, w_second, bias_pair, w_last = params

        def step(carry, blk):
            xrows, trow = blk
            pre_one = jnp.dot(xrows, w_first, preferred_element_type=jnp.float32) + bias_pair[0]
            act_one = jax.nn.silu(pre_one).astype(jnp.bfloat16)
            pre_two = jnp.dot(act_one, w_second, preferred_element_type=jnp.float32) + bias_pair[1]
            act_two = jax.nn.silu(pre_two).astype(jnp.bfloat16)
            q_row = jnp.dot(act_two.astype(jnp.float32), w_last.astype(jnp.float32), precision=high)
            error = q_row - trow
            delta_two = (error[:, None] * w_last.astype(jnp.float32)[None, :] * silu_slope(pre_two)).astype(jnp.bfloat16)
            back = jnp.dot(delta_two, w_second.T, preferred_element_type=jnp.float32)
            delta_one = (back * silu_slope(pre_one)).astype(jnp.bfloat16)
            part_in = jnp.dot(xrows.T, delta_one, preferred_element_type=jnp.float32)
            part_mid = jnp.dot(act_one.T, delta_two, preferred_element_type=jnp.float32)
            part_bias = jnp.stack([jnp.sum(delta_one.astype(jnp.float32), axis=0), jnp.sum(delta_two.astype(jnp.float32), axis=0)])
            part_out = jnp.dot(error, act_two.astype(jnp.float32), precision=high)
            sums = (carry[0] + rounded(part_in), carry[1] + rounded(part_mid), carry[2] + rounded(part_bias), carry[3] + rounded(part_out))
            return sums, q_row

        start = (jnp.zeros((width_in, hidden), jnp.float32), jnp.zeros((hidden, hidden), jnp.float32),
                 jnp.zeros((2, hidden), jnp.float32), jnp.zeros((hidden,), jnp.float32))
        sums, q_rows = lax.scan(step, start, (feat_blocks, target_blocks))
        return sums[0], sums[1], sums[2], sums[3], q_rows.reshape(total)

    grad_in, grad_mid, grad_bias, grad_out, q_values = lax.map(
        head_pass, (w_in, w_mid, jnp.transpose(biases, (1, 0, 2)), w_out))
    q_min = jnp.min(q_values, axis=0)
    gap = q_min - value_now
    weight = jnp.where(gap < 0.0, 0.3, 0.7)
    value_grad = -2.0 * weight * gap
    return (value_grad, jnp.transpose(grad_in, (1, 0, 2)), jnp.transpose(grad_mid, (1, 0, 2)),
            jnp.transpose(grad_bias, (1, 0, 2)), grad_out)
```

```python
import functools

import jax
import jax.numpy as jnp
from jax import lax
from jax.experimental import pallas as pl
from jax.experimental.pallas import tpu as pltpu
from jax.sharding import PartitionSpec as P

MESH = pl.DeviceIdType.MESH


def dot(a, b):
    return jnp.dot(a, b, preferred_element_type=jnp.float32)


def sigmoid(v):
    return 0.5 * jnp.tanh(0.5 * v) + 0.5


def kernel(
    n, e, x_ref, reward_ref, done_ref, vnext_ref, vnow_ref, w_in_ref, w_mid_hbm, bias_ref,
    w_out_ref, vg_ref, din_ref, dmid_ref, dbias_ref, dout_ref,
    w_mid, w_back, x_all, tgt_all, act_s, act2_s, g_s, delta_s, acc_mid, acc_in, stage, ibuf,
    qmin_s, qbuf, w_sem, xs_sem, xr_sem, ts_sem, tr_sem, is_sem, ir_sem, qs_sem, qr_sem,
):
    me = lax.axis_index("dp")
    my_ens = lax.axis_index("ens")
    rows, feats = x_ref.shape
    heads, _, units = w_in_ref.shape
    ks = units // n
    fs = feats // n
    chunk = min(512, units)
    chunks = units // chunk
    mine = pl.ds(pl.multiple_of(me * ks, ks), ks)

    loads = [
        pltpu.make_async_copy(w_mid_hbm.at[h], w_mid.at[h], w_sem.at[h]) for h in range(heads)
    ]
    for load in loads:
        load.start()

    barrier = pltpu.get_barrier_semaphore()
    for d in range(1, n):
        pl.semaphore_signal(
            barrier, inc=1, device_id={"dp": lax.rem(me + d, n)}, device_id_type=MESH
        )
    for d in range(1, e):
        pl.semaphore_signal(
            barrier, inc=1, device_id={"ens": lax.rem(my_ens + d, e)}, device_id_type=MESH
        )
    tgt_all[0] = reward_ref[...] + 0.99 * (1.0 - done_ref[...].astype(jnp.float32)) * vnext_ref[...]
    x_all[0] = x_ref[...]
    acc_mid[...] = jnp.zeros_like(acc_mid)
    acc_in[...] = jnp.zeros_like(acc_in)
    dbias_ref[...] = jnp.zeros_like(dbias_ref)
    dout_ref[...] = jnp.zeros_like(dout_ref)
    pl.semaphore_wait(barrier, n + e - 2)

    def send_x(d):
        return pltpu.make_async_remote_copy(
            src_ref=x_ref, dst_ref=x_all.at[d], send_sem=xs_sem.at[d], recv_sem=xr_sem.at[d],
            device_id={"dp": lax.rem(me + d, n)}, device_id_type=MESH,
        )

    def send_t(d):
        return pltpu.make_async_remote_copy(
            src_ref=tgt_all.at[0], dst_ref=tgt_all.at[d], send_sem=ts_sem.at[d],
            recv_sem=tr_sem.at[d], device_id={"dp": lax.rem(me + d, n)}, device_id_type=MESH,
        )

    def send_q(d):
        return pltpu.make_async_remote_copy(
            src_ref=qmin_s, dst_ref=qbuf.at[d], send_sem=qs_sem.at[d], recv_sem=qr_sem.at[d],
            device_id={"ens": lax.rem(my_ens + d, e)}, device_id_type=MESH,
        )

    def send_in(d):
        peer = lax.rem(me + d, n)
        return pltpu.make_async_remote_copy(
            src_ref=stage.at[:, pl.ds(pl.multiple_of(peer * fs, fs), fs), :],
            dst_ref=ibuf.at[d], send_sem=is_sem.at[d], recv_sem=ir_sem.at[d],
            device_id={"dp": peer}, device_id_type=MESH,
        )

    for d in range(1, n):
        send_x(d).start()
        send_t(d).start()

    diag = lax.broadcasted_iota(jnp.int32, (rows, rows), 0) == lax.broadcasted_iota(
        jnp.int32, (rows, rows), 1
    )

    def step(t, carry):
        @pl.when(t > 0)
        def _():
            send_x(t).wait_recv()
            send_t(t).wait_recv()

        @pl.when(t == 1)
        def _():
            for d in range(1, e):
                send_q(d).start()

        x = x_all[t]
        x_t = x.T
        tgt = jnp.sum(jnp.where(diag, tgt_all[t], 0.0), axis=1, keepdims=True)

        def head(h, carry):
            for c in range(chunks):
                cols = pl.ds(c * chunk, chunk)
                v = dot(x, w_in_ref[h, :, cols]) + bias_ref[0, h, :, cols]
                act_s[:, cols] = (v * sigmoid(v)).astype(jnp.bfloat16)

            @pl.when(t == 0)
            def _():
                pltpu.make_async_copy(w_mid_hbm.at[h], w_mid.at[h], w_sem.at[h]).wait()
                w_back[h] = w_mid[h, mine, :].T

            q = jnp.zeros((rows, 1), jnp.float32)
            for c in range(chunks):
                cols = pl.ds(c * chunk, chunk)
                v = dot(act_s[...], w_mid[h, :, cols]) + bias_ref[1, h, :, cols]
                s = sigmoid(v)
                a = v * s
                rounded = a.astype(jnp.bfloat16)
                act2_s[:, cols] = rounded
                wo = w_out_ref[h, :, cols]
                q += jnp.sum(rounded.astype(jnp.float32) * wo, axis=1, keepdims=True)
                g_s[:, cols] = (s + a * (1.0 - s)) * wo

            @pl.when(t == 0)
            def _():
                q_row = jnp.sum(jnp.where(diag, q, 0.0), axis=0, keepdims=True)
                qmin_s[...] = jnp.where(h == 0, q_row, jnp.minimum(q_row, qmin_s[...]))

            err = q - tgt
            act_t = act_s[:, mine].T
            back = jnp.zeros((rows, ks), jnp.float32)
            for c in range(chunks):
                cols = pl.ds(c * chunk, chunk)
                delta = (err * g_s[:, cols]).astype(jnp.bfloat16)
                delta_s[:, cols] = delta
                back += dot(delta, w_back[h, cols, :])
                acc_mid[h, :, cols] += dot(act_t, delta)
            v = dot(x, w_in_ref[h, :, mine]) + bias_ref[0, h, :, mine]
            s = sigmoid(v)
            delta_one = (back * (s + v * s * (1.0 - s))).astype(jnp.bfloat16)
            acc_in[h] += dot(x_t, delta_one)
            dbias_ref[0, h] += jnp.sum(delta_one.astype(jnp.float32), axis=0, keepdims=True)
            dbias_ref[1, h] += jnp.sum(
                delta_s[:, mine].astype(jnp.float32), axis=0, keepdims=True
            )
            dout_ref[h] += jnp.sum(
                err * act2_s[:, mine].astype(jnp.float32), axis=0, keepdims=True
            )
            return carry

        return lax.fori_loop(0, heads, head, carry)

    lax.fori_loop(0, n, step, 0)

    stage[...] = acc_in[...].astype(jnp.bfloat16)
    dmid_ref[...] = acc_mid[...].astype(jnp.bfloat16)
    for d in range(1, n):
        send_in(d).start()
    for h in range(heads):
        din_ref[h, :, mine] = acc_in[h, pl.ds(pl.multiple_of(me * fs, fs), fs), :]
    for d in range(1, e):
        send_q(d).wait_recv()
    q_min = qmin_s[...]
    for d in range(1, e):
        q_min = jnp.minimum(q_min, qbuf[d])
    gap = q_min - vnow_ref[...]
    vg_ref[...] = -2.0 * jnp.where(gap < 0.0, 0.3, 0.7) * gap
    for d in range(1, n):
        send_in(d).wait_recv()
        owner = lax.rem(me + n - d, n)
        for h in range(heads):
            din_ref[h, :, pl.ds(pl.multiple_of(owner * ks, ks), ks)] = ibuf[d, h].astype(
                jnp.float32
            )
    for d in range(1, n):
        send_x(d).wait_send()
        send_t(d).wait_send()
        send_in(d).wait_send()
    for d in range(1, e):
        send_q(d).wait_send()


def per_device(
    n, e, features, reward, done, value_next, value_now, w_in, w_mid, biases, w_out
):
    rows, feats = features.shape
    heads, _, units = w_in.shape
    ks, fs = units // n, feats // n
    f32, bf16 = jnp.float32, jnp.bfloat16
    vmem = pl.BlockSpec(memory_space=pltpu.VMEM)
    dma = pltpu.SemaphoreType.DMA
    vg, d_in, d_mid, d_bias, d_out = pl.pallas_call(
        functools.partial(kernel, n, e),
        out_shape=(
            jax.ShapeDtypeStruct((1, rows), f32),
            jax.ShapeDtypeStruct((heads, fs, units), f32),
            jax.ShapeDtypeStruct((heads, ks, units), bf16),
            jax.ShapeDtypeStruct((2, heads, 1, ks), f32),
            jax.ShapeDtypeStruct((heads, 1, ks), f32),
        ),
        in_specs=[vmem] * 6 + [pl.BlockSpec(memory_space=pl.ANY)] + [vmem] * 2,
        out_specs=(vmem,) * 5,
        scratch_shapes=[
            pltpu.VMEM((heads, units, units), bf16),
            pltpu.VMEM((heads, units, ks), bf16),
            pltpu.VMEM((n, rows, feats), bf16),
            pltpu.VMEM((n, 1, rows), f32),
            pltpu.VMEM((rows, units), bf16),
            pltpu.VMEM((rows, units), bf16),
            pltpu.VMEM((rows, units), f32),
            pltpu.VMEM((rows, units), bf16),
            pltpu.VMEM((heads, ks, units), f32),
            pltpu.VMEM((heads, feats, ks), f32),
            pltpu.VMEM((heads, feats, ks), bf16),
            pltpu.VMEM((n, heads, fs, ks), bf16),
            pltpu.VMEM((1, rows), f32),
            pltpu.VMEM((e, 1, rows), f32),
            dma((heads,)),
            dma((n,)), dma((n,)), dma((n,)), dma((n,)), dma((n,)), dma((n,)),
            dma((e,)), dma((e,)),
        ],
        compiler_params=pltpu.CompilerParams(
            collective_id=0, has_side_effects=True, vmem_limit_bytes=62 * 1024 * 1024
        ),
    )(
        features, reward[None], done[None], value_next[None], value_now[None], w_in, w_mid,
        biases[:, :, None, :], w_out.astype(f32)[:, None, :],
    )
    return (
        vg[0],
        jnp.transpose(d_in, (1, 0, 2)),
        jnp.transpose(d_mid, (1, 0, 2)).astype(f32),
        d_bias[:, :, 0, :],
        d_out[:, 0, :],
    )


def solution(mesh):
    in_specs = (
        P("dp", None),
        P("dp"),
        P("dp"),
        P("dp"),
        P("dp"),
        P("ens", None, None),
        P("ens", None, None),
        P(None, "ens", None),
        P("ens", None),
    )
    out_specs = (
        P("dp"),
        P("dp", "ens", None),
        P("dp", "ens", None),
        P(None, "ens", "dp"),
        P("ens", "dp"),
    )
    body = functools.partial(per_device, mesh.shape["dp"], mesh.shape["ens"])
    return jax.shard_map(
        body, mesh=mesh, in_specs=in_specs, out_specs=out_specs, check_vma=False
    )
```
